32 devices in a mesh: dp: 8 (over z, y), vocab: 4 (over x, core).
Axes of the slice: x: 2, y: 2, z: 4, core: 2. Of those that a mesh axis runs over, the one named last changes fastest.
Arguments:
- hidden_states: bfloat16 [4096, 2048], P('dp', 'vocab'), may hold values from -12 to 12
- teacher_logits: bfloat16 [4096, 16384], P('dp', 'vocab'), may hold values from -24 to 240
- head_weight: bfloat16 [2048, 16384], P(None, 'vocab'), as said below
Outputs:
- kl_per_token: float32 [4096], P('dp')
- hidden_grad: bfloat16 [4096, 2048], P('dp', 'vocab')
- head_grad: float32 [2048, 16384], P('dp', 'vocab')
The draws below stay inside these ranges and needn't reach their ends.
Inputs may be any that keep to these rules, and one draw needn't show every extreme that they name: `head_weight`: every entry's magnitude is at most 18 / sqrt(2048).
All inputs are finite; a program needn't handle non-finite values.
Results may differ from the reference program's by a relative error of at most 0.014.
Values may be sent and summed in bfloat16 or wider, within the bound.
A program may use at most 128 MiB of HBM per device.

```python
import math
import jax
import jax.numpy as jnp
from jax import lax

D = 2048
V = 16384
MICRO = 2
TOK = 256
TOKENS = 4096
N_DP = 8


def head_columns(key):
    column_key = jax.random.fold_in(key, 7101)
    value_key = jax.random.fold_in(column_key, 1)
    spread = 3.0 / math.sqrt(D)
    values = jnp.clip(jax.random.normal(value_key, (D, V), jnp.float32), -6.0, 6.0)
    return values * spread


def draw_head_weight(key, part):
    return head_columns(key).astype(jnp.bfloat16)


def draw_hidden_states(key, part):
    streams = jax.random.split(jax.random.fold_in(key, 7202), 2)
    values = jnp.clip(jax.random.normal(streams[1], (TOKENS, D), jnp.float32), -6.0, 6.0)
    return values.astype(jnp.bfloat16)


def draw_teacher_logits(key, part):
    streams = jax.random.split(jax.random.fold_in(key, 7303), 3)
    values = 3.0 * jnp.clip(jax.random.normal(streams[2], (TOKENS, V), jnp.float32), -8.0, 8.0)
    return values.astype(jnp.bfloat16)


def setup_inputs(seed: int = 0) -> dict:
    key_list = jax.random.split(jax.random.key(seed), 4)
    hidden_states = draw_hidden_states(jax.random.fold_in(key_list[3], 71), 0)
    teacher_logits = draw_teacher_logits(jax.random.fold_in(key_list[3], 71), 0)
    head_weight = draw_head_weight(jax.random.fold_in(key_list[3], 71), 0)
    return {"hidden_states": hidden_states, "teacher_logits": teacher_logits, "head_weight": head_weight}


grad_scale = 8.0


def token_group(hidden_rows, teacher_rows, head_weight):
    student = jnp.dot(hidden_rows, head_weight, preferred_element_type=jnp.float32)
    teacher = teacher_rows.astype(jnp.float32)
    student_max = jnp.max(student, axis=1, keepdims=True)
    teacher_max = jnp.max(teacher, axis=1, keepdims=True)
    student_terms = jnp.exp(student - student_max)
    teacher_terms = jnp.exp(teacher - teacher_max)
    student_total = jnp.sum(student_terms, axis=1)
    teacher_total = jnp.sum(teacher_terms, axis=1)
    cross_term = jnp.sum(teacher_terms * (teacher - student), axis=1)
    divergence = cross_term / teacher_total - teacher_max[:, 0] - jnp.log(teacher_total) + student_max[:, 0] + jnp.log(student_total)
    logit_grad = (grad_scale * (student_terms / student_total[:, None] - teacher_terms / teacher_total[:, None])).astype(jnp.bfloat16)
    hidden_grad = lax.dot_general(logit_grad, head_weight, (((1,), (1,)), ((), ())), preferred_element_type=jnp.float32).astype(jnp.bfloat16)
    group_grad = lax.dot_general(hidden_rows, logit_grad, (((0,), (0,)), ((), ())), preferred_element_type=jnp.float32).astype(jnp.bfloat16)
    return divergence, hidden_grad, group_grad


def reference(hidden_states, teacher_logits, head_weight):
    group_rows = MICRO * TOK
    grouped_hidden = hidden_states.reshape(N_DP, group_rows, D)
    grouped_teacher = teacher_logits.reshape(N_DP, group_rows, V)

    def one_group(running, inputs):
        divergence, hidden_grad, group_grad = token_group(inputs[0], inputs[1], head_weight)
        running = running + lax.optimization_barrier(group_grad).astype(jnp.float32)
        return running, (divergence, hidden_grad)

    head_grad, results = lax.scan(one_group, jnp.zeros((D, V), jnp.float32), (grouped_hidden, grouped_teacher))
    divergence = results[0].reshape(TOKENS)
    hidden_grad = results[1].reshape(TOKENS, D)
    return divergence, hidden_grad, head_grad
```

```python
import functools

import jax
import jax.numpy as jnp
from jax import lax
from jax.experimental import pallas as pl
from jax.experimental.pallas import tpu as pltpu
from jax.sharding import PartitionSpec as P

grad_scale = 8.0
PAIR = 2
MESH = pl.DeviceIdType.MESH


def slice_order(line):
    order = []
    low, high = 0, line - 1
    while low <= high:
        order.append(high)
        if low < high:
            order.append(low)
        low, high = low + 1, high - 1
    return order


def head_grad_kernel(
    line, chunks, width, rows, half,
    features_ref, grad_ref, out_ref,
    partner_grad, block, outgoing, incoming,
    pair_send, pair_recv, line_send, line_recv,
):
    me = lax.axis_index("dp")
    place = me // PAIR
    side = me - place * PAIR
    partner = place * PAIR + (PAIR - 1) - side
    has_down = place > 0
    has_up = place < line - 1
    up = jnp.where(has_up, me + PAIR, me)
    down = jnp.where(has_down, me - PAIR, me)

    barrier = pltpu.get_barrier_semaphore()
    pl.semaphore_signal(barrier, inc=1, device_id={"dp": partner}, device_id_type=MESH)

    @pl.when(has_down)
    def _():
        pl.semaphore_signal(barrier, inc=1, device_id={"dp": down}, device_id_type=MESH)

    @pl.when(has_up)
    def _():
        pl.semaphore_signal(barrier, inc=1, device_id={"dp": up}, device_id_type=MESH)

    pl.semaphore_wait(barrier, 1 + has_down.astype(jnp.int32) + has_up.astype(jnp.int32))

    def columns_of(chunk):
        return pl.ds(pl.multiple_of(chunk * width, width), width)

    def pair_copy(chunk):
        columns = columns_of(chunk)
        return pltpu.make_async_remote_copy(
            src_ref=grad_ref.at[:, columns],
            dst_ref=partner_grad.at[:, columns],
            send_sem=pair_send.at[chunk],
            recv_sem=pair_recv.at[chunk],
            device_id={"dp": partner},
            device_id_type=MESH,
        )

    def line_copy(chunk, part, slot, target):
        columns = columns_of(chunk)
        return pltpu.make_async_remote_copy(
            src_ref=outgoing.at[part, :, columns],
            dst_ref=incoming.at[slot, :, columns],
            send_sem=line_send.at[part, chunk],
            recv_sem=line_recv.at[slot, chunk],
            device_id={"dp": target},
            device_id_type=MESH,
        )

    @pl.loop(0, chunks)
    def _(chunk):
        pair_copy(chunk).start()

    def forward(chunk, part, has_source, slot, target):
        columns = columns_of(chunk)

        @pl.when(has_source)
        def _():
            line_copy(chunk, part, part, target).wait_recv()
            outgoing[part, :, columns] = (
                block[...] + incoming[part, :, columns].astype(jnp.float32)
            ).astype(jnp.bfloat16)

        @pl.when(jnp.logical_not(has_source))
        def _():
            outgoing[part, :, columns] = block[...].astype(jnp.bfloat16)

        line_copy(chunk, part, slot, target).start()

    def finish(chunk):
        columns = columns_of(chunk)

        @pl.when(has_down)
        def _():
            line_copy(chunk, 0, place, down).wait_recv()
            out_ref[:, columns] += incoming[place, :, columns].astype(jnp.float32)

        @pl.when(has_up)
        def _():
            line_copy(chunk, 0, line, up).wait_recv()
            out_ref[:, columns] += incoming[line, :, columns].astype(jnp.float32)

    lag = min(2, chunks)

    @pl.loop(0, chunks)
    def _(chunk):
        pair_copy(chunk).wait_recv()
        columns = columns_of(chunk)
        for part in slice_order(line):
            begin = part * rows
            block[...] = jnp.dot(
                features_ref[begin : begin + rows, :half],
                grad_ref[:, columns],
                preferred_element_type=jnp.float32,
            ) + jnp.dot(
                features_ref[begin : begin + rows, half:],
                partner_grad[:, columns],
                preferred_element_type=jnp.float32,
            )

            @pl.when(place == part)
            def _():
                out_ref[:, columns] = block[...]

            @pl.when(place < part)
            def _():
                forward(chunk, part, has_down, part, up)

            @pl.when(place > part)
            def _():
                forward(chunk, part, has_up, jnp.where(place - 1 == part, line, part), down)

        @pl.when(chunk >= lag)
        def _():
            finish(chunk - lag)

    @pl.loop(chunks - lag, chunks)
    def _(chunk):
        finish(chunk)

    @pl.loop(0, chunks)
    def _(chunk):
        pair_copy(chunk).wait_send()
        for part in range(line):

            @pl.when(place < part)
            def _():
                line_copy(chunk, part, part, up).wait_send()

            @pl.when(place > part)
            def _():
                line_copy(chunk, part, part, down).wait_send()


def reduce_head_grad(features, logit_grad, shards):
    line = shards // PAIR
    rows = features.shape[0] // line
    half, local_vocab = logit_grad.shape
    width = 256
    chunks = local_vocab // width
    return pl.pallas_call(
        functools.partial(head_grad_kernel, line, chunks, width, rows, half),
        out_shape=jax.ShapeDtypeStruct((rows, local_vocab), jnp.float32),
        in_specs=[pl.BlockSpec(memory_space=pltpu.VMEM)] * 2,
        out_specs=pl.BlockSpec(memory_space=pltpu.VMEM),
        scratch_shapes=[
            pltpu.VMEM((half, local_vocab), jnp.bfloat16),
            pltpu.VMEM((rows, width), jnp.float32),
            pltpu.VMEM((line, rows, local_vocab), jnp.bfloat16),
            pltpu.VMEM((line + 1, rows, local_vocab), jnp.bfloat16),
            pltpu.SemaphoreType.DMA((chunks,)),
            pltpu.SemaphoreType.DMA((chunks,)),
            pltpu.SemaphoreType.DMA((line, chunks)),
            pltpu.SemaphoreType.DMA((line + 1, chunks)),
        ],
        compiler_params=pltpu.CompilerParams(collective_id=0, has_side_effects=True),
    )(features, logit_grad)


def per_device(shards, hidden_states, teacher_logits, head_weight):
    tokens = hidden_states.shape[0]
    model_width = head_weight.shape[0]
    line = shards // PAIR
    rows = model_width // shards
    side = lax.axis_index("dp") % PAIR

    gathered = lax.all_gather(hidden_states, "vocab", axis=1, tiled=True)

    def slices(parity):
        return jnp.concatenate(
            [
                lax.dynamic_slice_in_dim(gathered, (part * PAIR + parity) * rows, rows, axis=1)
                for part in range(line)
            ],
            axis=1,
        )

    kept, given = slices(side), slices(1 - side)
    swap = [(index, index + 1 - 2 * (index % PAIR)) for index in range(shards)]
    received = lax.ppermute(given, "dp", swap)
    features = jnp.concatenate([kept.T, received.T], axis=1)

    student = jnp.dot(gathered, head_weight, preferred_element_type=jnp.float32)
    teacher = teacher_logits.astype(jnp.float32)
    student_top = jnp.max(student, axis=1)
    teacher_top = jnp.max(teacher, axis=1)
    teacher_terms = jnp.exp(teacher - teacher_top[:, None])
    stats = jnp.stack(
        [
            student_top,
            teacher_top,
            jnp.sum(jnp.exp(student - student_top[:, None]), axis=1),
            jnp.sum(teacher_terms, axis=1),
            jnp.sum(teacher_terms * (teacher - student), axis=1),
        ]
    )
    stats = lax.all_gather(stats, "vocab", axis=0, tiled=False)
    student_max = jnp.max(stats[:, 0], axis=0)
    teacher_max = jnp.max(stats[:, 1], axis=0)
    student_scale = jnp.exp(stats[:, 0] - student_max)
    teacher_scale = jnp.exp(stats[:, 1] - teacher_max)
    student_total = jnp.sum(stats[:, 2] * student_scale, axis=0)
    teacher_total = jnp.sum(stats[:, 3] * teacher_scale, axis=0)
    cross_term = jnp.sum(stats[:, 4] * teacher_scale, axis=0)
    student_log = student_max + jnp.log(student_total)
    teacher_log = teacher_max + jnp.log(teacher_total)
    divergence = cross_term / teacher_total - teacher_log + student_log
    logit_grad = (
        grad_scale
        * (jnp.exp(student - student_log[:, None]) - jnp.exp(teacher - teacher_log[:, None]))
    ).astype(jnp.bfloat16)
    logit_grad, features = lax.optimization_barrier((logit_grad, features))
    partial_value = lax.dot_general(
        logit_grad, head_weight, (((1,), (1,)), ((), ())), preferred_element_type=jnp.float32
    ).astype(jnp.bfloat16)
    partial_value, logit_grad = lax.optimization_barrier((partial_value, logit_grad))
    hidden_grad = lax.psum_scatter(partial_value, "vocab", scatter_dimension=1, tiled=True)
    head_grad = reduce_head_grad(features, logit_grad, shards)
    return (divergence, hidden_grad, head_grad)


def solution(mesh):
    in_specs = (P("dp", "vocab"), P("dp", "vocab"), P(None, "vocab"))
    out_specs = (P("dp"), P("dp", "vocab"), P("dp", "vocab"))
    return jax.shard_map(
        functools.partial(per_device, mesh.shape["dp"]),
        mesh=mesh, in_specs=in_specs, out_specs=out_specs, check_vma=False,
    )
```

```python
import functools

import jax
import jax.numpy as jnp
from jax import lax
from jax.experimental import pallas as pl
from jax.experimental.pallas import tpu as pltpu
from jax.sharding import PartitionSpec as P

grad_scale = 8.0
PAIR = 2
MESH = pl.DeviceIdType.MESH


def slice_order(line):
    order = []
    low, high = 0, line - 1
    while low <= high:
        order.append(high)
        if low < high:
            order.append(low)
        low, high = low + 1, high - 1
    return order


def head_grad_kernel(
    line, chunks, width, rows, half,
    features_ref, grad_ref, out_ref,
    partner_grad, block, outgoing, incoming,
    pair_send, pair_recv, line_send, line_recv,
):
    me = lax.axis_index("dp")
    place = me // PAIR
    side = me - place * PAIR
    partner = place * PAIR + (PAIR - 1) - side
    has_down = place > 0
    has_up = place < line - 1
    up = jnp.where(has_up, me + PAIR, me)
    down = jnp.where(has_down, me - PAIR, me)

    barrier = pltpu.get_barrier_semaphore()
    pl.semaphore_signal(barrier, inc=1, device_id={"dp": partner}, device_id_type=MESH)

    @pl.when(has_down)
    def _():
        pl.semaphore_signal(barrier, inc=1, device_id={"dp": down}, device_id_type=MESH)

    @pl.when(has_up)
    def _():
        pl.semaphore_signal(barrier, inc=1, device_id={"dp": up}, device_id_type=MESH)

    pl.semaphore_wait(barrier, 1 + has_down.astype(jnp.int32) + has_up.astype(jnp.int32))

    def columns_of(chunk):
        return pl.ds(pl.multiple_of(chunk * width, width), width)

    def pair_copy(chunk):
        columns = columns_of(chunk)
        return pltpu.make_async_remote_copy(
            src_ref=grad_ref.at[:, columns],
            dst_ref=partner_grad.at[:, columns],
            send_sem=pair_send.at[chunk],
            recv_sem=pair_recv.at[chunk],
            device_id={"dp": partner},
            device_id_type=MESH,
        )

    def line_copy(chunk, part, slot, target):
        columns = columns_of(chunk)
        return pltpu.make_async_remote_copy(
            src_ref=outgoing.at[part, :, columns],
            dst_ref=incoming.at[slot, :, columns],
            send_sem=line_send.at[part, chunk],
            recv_sem=line_recv.at[slot, chunk],
            device_id={"dp": target},
            device_id_type=MESH,
        )

    ahead = min(3, chunks)
    window = min(2, chunks)

    @pl.loop(0, ahead)
    def _(chunk):
        pair_copy(chunk).start()

    def drain(chunk):
        for part in range(line):

            @pl.when(place < part)
            def _():
                line_copy(chunk, part, part, up).wait_send()

            @pl.when(place > part)
            def _():
                line_copy(chunk, part, part, down).wait_send()

    def forward(chunk, part, has_source, slot, target):
        columns = columns_of(chunk)

        @pl.when(has_source)
        def _():
            line_copy(chunk, part, part, target).wait_recv()
            outgoing[part, :, columns] = (
                block[...] + incoming[part, :, columns].astype(jnp.float32)
            ).astype(jnp.bfloat16)

        @pl.when(jnp.logical_not(has_source))
        def _():
            outgoing[part, :, columns] = block[...].astype(jnp.bfloat16)

        line_copy(chunk, part, slot, target).start()

    def finish(chunk):
        columns = columns_of(chunk)

        @pl.when(has_down)
        def _():
            line_copy(chunk, 0, place, down).wait_recv()
            out_ref[:, columns] += incoming[place, :, columns].astype(jnp.float32)

        @pl.when(has_up)
        def _():
            line_copy(chunk, 0, line, up).wait_recv()
            out_ref[:, columns] += incoming[line, :, columns].astype(jnp.float32)

    lag = min(2, chunks)

    @pl.loop(0, chunks)
    def _(chunk):
        pair_copy(chunk).wait_recv()

        @pl.when(chunk + ahead < chunks)
        def _():
            pair_copy(chunk + ahead).start()

        @pl.when(chunk >= window)
        def _():
            drain(chunk - window)

        columns = columns_of(chunk)
        for part in slice_order(line):
            begin = part * rows
            block[...] = jnp.dot(
                features_ref[begin : begin + rows, :half],
                grad_ref[:, columns],
                preferred_element_type=jnp.float32,
            ) + jnp.dot(
                features_ref[begin : begin + rows, half:],
                partner_grad[:, columns],
                preferred_element_type=jnp.float32,
            )

            @pl.when(place == part)
            def _():
                out_ref[:, columns] = block[...]

            @pl.when(place < part)
            def _():
                forward(chunk, part, has_down, part, up)

            @pl.when(place > part)
            def _():
                forward(chunk, part, has_up, jnp.where(place - 1 == part, line, part), down)

        @pl.when(chunk >= lag)
        def _():
            finish(chunk - lag)

    @pl.loop(chunks - lag, chunks)
    def _(chunk):
        finish(chunk)

    @pl.loop(chunks - window, chunks)
    def _(chunk):
        drain(chunk)

    @pl.loop(0, chunks)
    def _(chunk):
        pair_copy(chunk).wait_send()


def reduce_head_grad(features, logit_grad, shards):
    line = shards // PAIR
    rows = features.shape[0] // line
    half, local_vocab = logit_grad.shape
    width = 256
    chunks = local_vocab // width
    return pl.pallas_call(
        functools.partial(head_grad_kernel, line, chunks, width, rows, half),
        out_shape=jax.ShapeDtypeStruct((rows, local_vocab), jnp.float32),
        in_specs=[pl.BlockSpec(memory_space=pltpu.VMEM)] * 2,
        out_specs=pl.BlockSpec(memory_space=pltpu.VMEM),
        scratch_shapes=[
            pltpu.VMEM((half, local_vocab), jnp.bfloat16),
            pltpu.VMEM((rows, width), jnp.float32),
            pltpu.VMEM((line, rows, local_vocab), jnp.bfloat16),
            pltpu.VMEM((line + 1, rows, local_vocab), jnp.bfloat16),
            pltpu.SemaphoreType.DMA((chunks,)),
            pltpu.SemaphoreType.DMA((chunks,)),
            pltpu.SemaphoreType.DMA((line, chunks)),
            pltpu.SemaphoreType.DMA((line + 1, chunks)),
        ],
        compiler_params=pltpu.CompilerParams(collective_id=0, has_side_effects=True),
    )(features, logit_grad)


def per_device(shards, hidden_states, teacher_logits, head_weight):
    tokens = hidden_states.shape[0]
    model_width = head_weight.shape[0]
    line = shards // PAIR
    rows = model_width // shards
    side = lax.axis_index("dp") % PAIR

    gathered = lax.all_gather(hidden_states, "vocab", axis=1, tiled=True)

    def slices(parity):
        return jnp.concatenate(
            [
                lax.dynamic_slice_in_dim(gathered, (part * PAIR + parity) * rows, rows, axis=1)
                for part in range(line)
            ],
            axis=1,
        )

    kept, given = slices(side), slices(1 - side)
    swap = [(index, index + 1 - 2 * (index % PAIR)) for index in range(shards)]
    received = lax.ppermute(given, "dp", swap)

    student = jnp.dot(gathered, head_weight, preferred_element_type=jnp.float32)
    teacher = teacher_logits.astype(jnp.float32)
    student_top = jnp.max(student, axis=1)
    teacher_top = jnp.max(teacher, axis=1)
    teacher_terms = jnp.exp(teacher - teacher_top[:, None])
    stats = jnp.stack(
        [
            student_top,
            teacher_top,
            jnp.sum(jnp.exp(student - student_top[:, None]), axis=1),
            jnp.sum(teacher_terms, axis=1),
            jnp.sum(teacher_terms * (teacher - student), axis=1),
        ]
    )
    stats, received = lax.optimization_barrier((stats, received))
    stats = lax.all_gather(stats, "vocab", axis=0, tiled=False)
    features = jnp.concatenate([kept.T, received.T], axis=1)
    student_max = jnp.max(stats[:, 0], axis=0)
    teacher_max = jnp.max(stats[:, 1], axis=0)
    student_scale = jnp.exp(stats[:, 0] - student_max)
    teacher_scale = jnp.exp(stats[:, 1] - teacher_max)
    student_total = jnp.sum(stats[:, 2] * student_scale, axis=0)
    teacher_total = jnp.sum(stats[:, 3] * teacher_scale, axis=0)
    cross_term = jnp.sum(stats[:, 4] * teacher_scale, axis=0)
    student_log = student_max + jnp.log(student_total)
    teacher_log = teacher_max + jnp.log(teacher_total)
    divergence = cross_term / teacher_total - teacher_log + student_log
    logit_grad = (
        grad_scale
        * (jnp.exp(student - student_log[:, None]) - jnp.exp(teacher - teacher_log[:, None]))
    ).astype(jnp.bfloat16)
    logit_grad, features = lax.optimization_barrier((logit_grad, features))
    partial_value = lax.dot_general(
        logit_grad, head_weight, (((1,), (1,)), ((), ())), preferred_element_type=jnp.float32
    ).astype(jnp.bfloat16)
    partial_value, logit_grad = lax.optimization_barrier((partial_value, logit_grad))
    hidden_grad = lax.psum_scatter(partial_value, "vocab", scatter_dimension=1, tiled=True)
    head_grad = reduce_head_grad(features, logit_grad, shards)
    return (divergence, hidden_grad, head_grad)


def solution(mesh):
    in_specs = (P("dp", "vocab"), P("dp", "vocab"), P(None, "vocab"))
    out_specs = (P("dp"), P("dp", "vocab"), P("dp", "vocab"))
    return jax.shard_map(
        functools.partial(per_device, mesh.shape["dp"]),
        mesh=mesh, in_specs=in_specs, out_specs=out_specs, check_vma=False,
    )
```
